32 devices in a mesh: rows: 16 (over z, y, x), sub: 2 (over core).
Axes of the slice: x: 2, y: 2, z: 4, core: 2. Of those that a mesh axis runs over, the one named last changes fastest.
Arguments:
- matrix: float32 [4096, 384], P(('rows', 'sub')), as said below
- grad_out: float32 [4096, 384], P(('rows', 'sub')), as said below
- grad_factor: float32 [384, 384], replicated, may hold values from -6 to 6
Outputs:
- grad_matrix: float32 [4096, 384], P(('rows', 'sub'))
The draws below stay inside these ranges and needn't reach their ends.
Inputs may be any that keep to these rules, and one draw needn't show every extreme that they name: `matrix`: entries at most of order 1 / sqrt(4096), with a scale that varies by row and by column. `grad_out`: entries of order 0.01.
All inputs are finite; a program needn't handle non-finite values.
Results may differ from the reference program's by a relative error of at most 0.0004.
Values sent between devices are 32-bit elements; how exact they have to be, the bound alone decides.
A program may use at most 64 MiB of HBM per device.

```python
import jax
import jax.numpy as jnp
from jax import lax

N = 384
SECTIONS = 2
R_DEV = 128
ROWS = 4096


def column_mix(key):
    gaussian = jax.random.normal(jax.random.fold_in(key, 15), (N, N), jnp.float32)
    rotation = jnp.linalg.qr(gaussian)[0]
    position = jnp.arange(N, dtype=jnp.float32) / (N - 1)
    column_decay = jnp.power(jnp.float32(10.0), -4.0 * jnp.cbrt(position))
    return column_decay[:, None] * rotation


def shared_rows(key):
    blocks = ROWS // R_DEV
    base_rows = jax.random.normal(jax.random.fold_in(key, 11), (ROWS, N), jnp.float32)
    block_scale = jnp.exp(jax.random.uniform(jax.random.fold_in(key, 13), (blocks, 1), jnp.float32, -0.7, 0.7))
    row_scale = jnp.exp(jax.random.uniform(jax.random.fold_in(key, 14), (ROWS, 1), jnp.float32, -0.5, 0.5))
    scaled = jnp.repeat(block_scale, R_DEV, axis=0) * row_scale
    mixed = jnp.dot(base_rows * scaled, column_mix(key), precision=lax.Precision.HIGHEST, preferred_element_type=jnp.float32)
    return mixed / jnp.sqrt(jnp.float32(ROWS))


def draw_matrix(key, part):
    return shared_rows(key)


def draw_grad_out(key, part):
    noise_rows = jax.random.normal(jax.random.fold_in(key, 21), (ROWS, N), jnp.float32)
    return 0.01 * (noise_rows + 0.03 * jnp.sqrt(jnp.float32(ROWS)) * shared_rows(key))


def normal_values(stream_key, dims, scale, most, held_as=jnp.bfloat16):
    entries = jax.random.normal(stream_key, dims, jnp.float32) * scale
    return jnp.minimum(jnp.maximum(entries, -most), most).astype(held_as)


def setup_inputs(seed: int = 0) -> dict:
    arg_keys = jax.random.split(jax.random.key(seed), 4)
    return {
        "matrix": draw_matrix(jax.random.fold_in(arg_keys[3], 71), 0),
        "grad_out": draw_grad_out(jax.random.fold_in(arg_keys[3], 71), 0),
        "grad_factor": normal_values(arg_keys[2], (N, N), 1.0, 6.0, jnp.float32),
    }


shift_frac = 0.02

def full_dot(left, right):
    return jnp.dot(left.astype(jnp.float32), right.astype(jnp.float32), precision=lax.Precision.HIGHEST, preferred_element_type=jnp.float32)

def inner_gram(left, right):
    return lax.dot_general(left.astype(jnp.float32), right.astype(jnp.float32), (((0,), (0,)), ((), ())), precision=lax.Precision.HIGHEST, preferred_element_type=jnp.float32)

def cholesky_adjoint(lower_fac, lower_inv, lower_grad):
    product = full_dot(lower_fac.T, lower_grad)
    phi_part = jnp.tril(product) - 0.5 * jnp.diag(jnp.diag(product))
    sandwich = full_dot(full_dot(lower_inv.T, phi_part), lower_inv)
    return 0.5 * (sandwich + sandwich.T)

def factor_grads(uppers, grad_factor):
    count = len(uppers)
    result = []
    for section_index in range(count):
        middle = grad_factor
        for later in range(section_index + 1, count):
            middle = full_dot(uppers[later].T, middle)
        for earlier in range(section_index - 1, -1, -1):
            middle = full_dot(middle, uppers[earlier].T)
        result.append(middle)
    return result

def reference(matrix, grad_out, grad_factor):
    width = matrix.shape[1]
    rate = shift_frac / width
    identity = jnp.eye(width, dtype=jnp.float32)
    current = matrix
    saved = []
    for section_index in range(SECTIONS):
        summed = inner_gram(current, current)
        shift_val = rate * jnp.trace(summed)
        lower_fac = jnp.linalg.cholesky(summed + shift_val * identity)
        lower_inv = lax.linalg.triangular_solve(lower_fac, identity, left_side=True, lower=True)
        following = full_dot(current, lower_inv.T)
        saved.append((current, following, lower_fac, lower_inv))
        current = following
    uppers = [item[2].T for item in saved]
    fac_grads = factor_grads(uppers, grad_factor)
    q_grad = grad_out
    for section_index in range(SECTIONS - 1, -1, -1):
        before, after, lower_fac, lower_inv = saved[section_index]
        crossed = inner_gram(after, q_grad)
        total_grad = fac_grads[section_index] - full_dot(crossed, lower_inv)
        gram_grad = cholesky_adjoint(lower_fac, lower_inv, jnp.tril(total_grad.T))
        gram_grad = gram_grad + rate * jnp.trace(gram_grad) * identity
        q_grad = full_dot(q_grad, lower_inv) + 2.0 * full_dot(before, gram_grad)
    return q_grad
```

```python
import functools

import jax
import jax.numpy as jnp
from jax import lax
from jax.experimental import pallas as pl
from jax.experimental.pallas import tpu as pltpu
from jax.sharding import PartitionSpec as P

LANES = 128
PANEL = 8
shift_frac = 0.02
VMEM_LIMIT = 56 * 1024 * 1024


def dot(left, right, dims=((1,), (0,))):
    return lax.dot_general(
        left, right, (dims, ((), ())), precision=lax.Precision.HIGHEST, preferred_element_type=jnp.float32
    )


def dot_tn(left, right):
    return dot(left, right, ((0,), (0,)))


def dot_nt(left, right):
    return dot(left, right, ((1,), (1,)))


def upper_pairs(count):
    return [(i, j) for i in range(count) for j in range(i, count)]


def block(index):
    return pl.ds(index * LANES, LANES)


def iotas(shape):
    return lax.broadcasted_iota(jnp.int32, shape, 0), lax.broadcasted_iota(jnp.int32, shape, 1)


def piece_rows(rows, devices):
    share = -(-rows // devices)
    return -(-share // 8) * 8


class Summer:
    def __init__(self, counts, rows):
        self.counts = counts
        self.devices = counts[0] * counts[1]
        self.piece = piece_rows(rows, self.devices)
        self.owners = -(-rows // self.piece)
        self.rows = self.owners * self.piece

    def scratch(self):
        return [
            pltpu.VMEM((self.rows, LANES), jnp.float32),
            pltpu.VMEM((self.devices - 1, self.piece, LANES), jnp.float32),
            pltpu.VMEM((self.rows, LANES), jnp.float32),
            pltpu.SemaphoreType.DMA((4,)),
        ]

    def bind(self, me, part, inbox, total, sems):
        self.me, self.part, self.inbox, self.total, self.sems = me, part, inbox, total, sems
        return self

    def peer(self, offset):
        return lax.rem(self.me + offset, self.devices)

    def place(self, device):
        return (device // self.counts[1], lax.rem(device, self.counts[1]))

    def rows_of(self, device):
        return pl.ds(pl.multiple_of(device * self.piece, 8), self.piece)

    def is_owner(self, device, action):
        if self.owners == self.devices:
            action()
        else:
            pl.when(device < self.owners)(action)

    def greet(self):
        barrier = pltpu.get_barrier_semaphore()

        def signal(offset, carry):
            pl.semaphore_signal(
                barrier, inc=1, device_id=self.place(self.peer(offset)), device_id_type=pl.DeviceIdType.MESH
            )
            return carry

        lax.fori_loop(1, self.devices, signal, 0)

    def greeted(self):
        pl.semaphore_wait(pltpu.get_barrier_semaphore(), self.devices - 1)

    def outgoing(self, offset):
        peer = self.peer(offset)
        return pltpu.make_async_remote_copy(
            src_ref=self.part.at[self.rows_of(peer)],
            dst_ref=self.inbox.at[offset - 1],
            send_sem=self.sems.at[0],
            recv_sem=self.sems.at[1],
            device_id=self.place(peer),
            device_id_type=pl.DeviceIdType.MESH,
        )

    def spread(self, offset):
        mine = self.total.at[self.rows_of(self.me)]
        return pltpu.make_async_remote_copy(
            src_ref=mine,
            dst_ref=mine,
            send_sem=self.sems.at[2],
            recv_sem=self.sems.at[3],
            device_id=self.place(self.peer(offset)),
            device_id_type=pl.DeviceIdType.MESH,
        )

    def each_peer(self, action):
        def step(offset, carry):
            action(offset)
            return carry

        lax.fori_loop(1, self.devices, step, 0)

    def start(self):
        self.each_peer(lambda offset: self.is_owner(self.peer(offset), lambda: self.outgoing(offset).start()))

    def reduce(self):
        def owned():
            pltpu.make_async_copy(self.inbox, self.inbox, self.sems.at[1]).wait()
            mine = self.rows_of(self.me)
            summed = self.part[mine, :]
            for slot in range(self.devices - 1):
                summed = summed + self.inbox[slot]
            self.total[mine, :] = summed
            self.each_peer(lambda offset: self.spread(offset).start())

        self.is_owner(self.me, owned)

    def wait_rows(self, rows):
        view = self.total.at[pl.ds(0, rows)]
        pltpu.make_async_copy(view, view, self.sems.at[3]).wait()

    def finish(self):
        if self.owners == self.devices:
            self.wait_rows(self.rows - self.piece)
        else:
            pl.when(self.me < self.owners)(lambda: self.wait_rows(self.rows - self.piece))
            pl.when(self.me >= self.owners)(lambda: self.wait_rows(self.rows))
        self.each_peer(lambda offset: self.is_owner(self.peer(offset), lambda: self.outgoing(offset).wait_send()))
        self.is_owner(self.me, lambda: self.each_peer(lambda offset: self.spread(offset).wait_send()))


def store_gram(part, source, pairs):
    for index, (i, j) in enumerate(pairs):
        part[block(index), :] = dot_tn(source[:, block(i)], source[:, block(j)])


def first_kernel(counts, pairs, matrix, gram, part, inbox, total, sems):
    me = lax.axis_index("rows") * counts[1] + lax.axis_index("sub")
    summer = Summer(counts, len(pairs) * LANES).bind(me, part, inbox, total, sems)
    summer.greet()
    store_gram(part, matrix, pairs)
    summer.greeted()
    summer.start()
    summer.reduce()
    summer.finish()
    gram[...] = total[pl.ds(0, len(pairs) * LANES), :]


def second_kernel(counts, pairs, current, q_grad, sums, part, inbox, total, sems):
    me = lax.axis_index("rows") * counts[1] + lax.axis_index("sub")
    width = current.shape[1] // LANES
    used = (len(pairs) + width * width) * LANES
    summer = Summer(counts, used).bind(me, part, inbox, total, sems)
    summer.greet()
    store_gram(part, current, pairs)
    for i in range(width):
        for j in range(width):
            slot = len(pairs) + i * width + j
            part[block(slot), :] = dot_tn(current[:, block(i)], q_grad[:, block(j)])
    if summer.rows > used:
        part[pl.ds(used, summer.rows - used), :] = jnp.zeros((summer.rows - used, LANES), jnp.float32)
    summer.greeted()
    summer.start()
    summer.reduce()
    summer.finish()
    sums[...] = total[pl.ds(0, used), :]


def factor_block(work):
    sub, lane = iotas((PANEL, LANES))

    def step(group, carry):
        top = group * PANEL
        rows = pl.ds(pl.multiple_of(top, PANEL), PANEL)
        left = work[rows, pl.ds(0, LANES)]
        right = work[rows, pl.ds(LANES, LANES)]
        rolled = pltpu.roll(left, lax.rem(LANES - top, LANES), 1)
        cols = [jnp.broadcast_to(rolled[:, k : k + 1], (PANEL, LANES)) for k in range(PANEL)]
        pivots = jnp.zeros((PANEL, LANES), jnp.float32)
        for k in range(PANEL):
            pivot = jnp.broadcast_to(cols[k][k : k + 1, :], (PANEL, LANES))
            pivots = jnp.where(sub == k, pivot, pivots)
            factor = jnp.where(sub > k, cols[k] / pivot, 0.0)
            for later in range(k + 1, PANEL):
                cols[later] = cols[later] - factor * jnp.broadcast_to(cols[later][k : k + 1, :], (PANEL, LANES))
            left = left - factor * jnp.broadcast_to(left[k : k + 1, :], (PANEL, LANES))
            right = right - factor * jnp.broadcast_to(right[k : k + 1, :], (PANEL, LANES))
        scale = 1.0 / jnp.sqrt(pivots)
        left = jnp.where(lane >= top + sub, left * scale, 0.0)
        right = right * scale
        both = jnp.concatenate([left, right], axis=1)
        below = jnp.where(lane >= top + PANEL, left, 0.0)
        work[...] = work[...] - dot_tn(below, both)
        work[rows, :] = both
        return carry

    lax.fori_loop(0, LANES // PANEL, step, 0)


def factor_all(width, gram, work, upper, inverse):
    pairs = upper_pairs(width)
    size = width * LANES
    rate = shift_frac / size
    row, lane = iotas((LANES, LANES))
    same = row == lane
    trace = jnp.float32(0.0)
    for index, (i, j) in enumerate(pairs):
        if i == j:
            trace = trace + jnp.sum(jnp.where(same, gram[block(index), :], 0.0))
    shift = rate * trace
    eye = jnp.where(same, 1.0, 0.0).astype(jnp.float32)
    zero = jnp.zeros((LANES, LANES), jnp.float32)
    for index, (i, j) in enumerate(pairs):
        piece = gram[block(index), :]
        upper[block(i), block(j)] = piece + shift * eye if i == j else piece
        if i != j:
            upper[block(j), block(i)] = zero
            inverse[block(i), block(j)] = zero
    for b in range(width):
        work[:, pl.ds(0, LANES)] = upper[block(b), block(b)]
        work[:, pl.ds(LANES, LANES)] = eye
        factor_block(work)
        upper[block(b), block(b)] = work[:, pl.ds(0, LANES)]
        inv = work[:, pl.ds(LANES, LANES)]
        inverse[block(b), block(b)] = inv
        for j in range(b + 1, width):
            upper[block(b), block(j)] = dot(inv, upper[block(b), block(j)])
        for i in range(b + 1, width):
            for j in range(i, width):
                upper[block(i), block(j)] = upper[block(i), block(j)] - dot_tn(
                    upper[block(b), block(i)], upper[block(b), block(j)]
                )
        for j in range(b):
            acc = zero
            for k in range(j, b):
                acc = acc + dot_tn(upper[block(k), block(b)], inverse[block(k), block(j)])
            inverse[block(b), block(j)] = -dot(inv, acc)


def section_kernel(width, gram, matrix, upper, inverse, following, work):
    factor_all(width, gram, work, upper, inverse)
    following[...] = dot_nt(matrix[...], inverse[...])


def gram_grad(upper, inverse, total_grad, rate):
    row, lane = iotas(total_grad.shape)
    lower_grad = jnp.where(row >= lane, total_grad.T, 0.0)
    product = dot(upper, lower_grad)
    phi = jnp.where(row > lane, product, jnp.where(row == lane, 0.5 * product, 0.0))
    sandwich = dot(dot_tn(inverse, phi), inverse)
    result = 0.5 * (sandwich + sandwich.T)
    trace = jnp.sum(jnp.where(row == lane, result, 0.0))
    return result + jnp.where(row == lane, rate * trace, 0.0)


def last_kernel(
    width, sums, upper1, inverse1, matrix, current, q_grad, grad_factor, out, work, upper2, inverse2, gram2, cross
):
    pairs = upper_pairs(width)
    rate = shift_frac / (width * LANES)
    factor_all(width, sums, work, upper2, inverse2)
    for index, (i, j) in enumerate(pairs):
        piece = sums[block(index), :]
        gram2[block(i), block(j)] = piece
        if i != j:
            gram2[block(j), block(i)] = piece.T
    for i in range(width):
        for j in range(width):
            cross[block(i), block(j)] = sums[block(len(pairs) + i * width + j), :]
    total2 = dot_nt(grad_factor[...], upper1[...]) - dot(dot(inverse2[...], cross[...]), inverse2[...])
    grad2 = gram_grad(upper2[...], inverse2[...], total2, rate)
    crossed1 = dot(cross[...], inverse2[...]) + 2.0 * dot(gram2[...], grad2)
    total1 = dot_tn(upper2[...], grad_factor[...]) - dot(crossed1, inverse1[...])
    grad1 = gram_grad(upper1[...], inverse1[...], total1, rate)
    middle = dot(q_grad[...], inverse2[...]) + 2.0 * dot(current[...], grad2)
    out[...] = dot(middle, inverse1[...]) + 2.0 * dot(matrix[...], grad1)


def per_device(counts, matrix, grad_out, grad_factor):
    rows, size = matrix.shape
    width = size // LANES
    pairs = upper_pairs(width)
    vmem = pl.BlockSpec(memory_space=pltpu.VMEM)
    square = jax.ShapeDtypeStruct((size, size), jnp.float32)
    tall = jax.ShapeDtypeStruct((rows, size), jnp.float32)
    square_scratch = pltpu.VMEM((size, size), jnp.float32)
    work = pltpu.VMEM((LANES, 2 * LANES), jnp.float32)

    def call(body, outs, args, scratch, **params):
        return pl.pallas_call(
            body,
            out_shape=outs,
            in_specs=[vmem] * len(args),
            out_specs=jax.tree.map(lambda _: vmem, outs),
            scratch_shapes=scratch,
            compiler_params=pltpu.CompilerParams(vmem_limit_bytes=VMEM_LIMIT, **params),
        )(*args)

    used = len(pairs) * LANES
    gram = call(
        functools.partial(first_kernel, counts, pairs),
        jax.ShapeDtypeStruct((used, LANES), jnp.float32),
        (matrix,),
        Summer(counts, used).scratch(),
        collective_id=0,
        has_side_effects=True,
    )
    upper1, inverse1, current = call(
        functools.partial(section_kernel, width), (square, square, tall), (gram, matrix), [work]
    )
    used = (len(pairs) + width * width) * LANES
    sums = call(
        functools.partial(second_kernel, counts, pairs),
        jax.ShapeDtypeStruct((used, LANES), jnp.float32),
        (current, grad_out),
        Summer(counts, used).scratch(),
        collective_id=1,
        has_side_effects=True,
    )
    return call(
        functools.partial(last_kernel, width),
        tall,
        (sums, upper1, inverse1, matrix, current, grad_out, grad_factor),
        [work] + [square_scratch] * 4,
    )


def solution(mesh):
    counts = (mesh.shape["rows"], mesh.shape["sub"])
    placed = (P(("rows", "sub"), None), P(("rows", "sub"), None), P())
    return jax.shard_map(
        functools.partial(per_device, counts),
        mesh=mesh,
        in_specs=placed,
        out_specs=P(("rows", "sub"), None),
        check_vma=False,
    )
```

```python
import functools

import jax
import jax.numpy as jnp
from jax import lax
from jax.experimental import pallas as pl
from jax.experimental.pallas import tpu as pltpu
from jax.sharding import PartitionSpec as P

LANES = 128
PANEL = 16
shift_frac = 0.02
VMEM_LIMIT = 56 * 1024 * 1024


def dot(left, right, dims=((1,), (0,))):
    return lax.dot_general(
        left, right, (dims, ((), ())), precision=lax.Precision.HIGHEST, preferred_element_type=jnp.float32
    )


def dot_tn(left, right):
    return dot(left, right, ((0,), (0,)))


def dot_nt(left, right):
    return dot(left, right, ((1,), (1,)))


def upper_pairs(count):
    return [(i, j) for i in range(count) for j in range(i, count)]


def block(index):
    return pl.ds(index * LANES, LANES)


def iotas(shape):
    return lax.broadcasted_iota(jnp.int32, shape, 0), lax.broadcasted_iota(jnp.int32, shape, 1)


def piece_rows(rows, devices):
    share = -(-rows // devices)
    return -(-share // 8) * 8


class Summer:
    def __init__(self, counts, rows):
        self.counts, self.used = counts, rows
        self.devices = counts[0] * counts[1]
        self.piece = piece_rows(rows, self.devices)
        self.owners = -(-rows // self.piece)
        self.rows = self.owners * self.piece

    def scratch(self):
        return [
            pltpu.VMEM((self.rows, LANES), jnp.float32),
            pltpu.VMEM((self.devices - 1, self.piece, LANES), jnp.float32),
            pltpu.VMEM((self.rows, LANES), jnp.float32),
            pltpu.SemaphoreType.DMA((4,)),
        ]

    def bind(self, me, part, inbox, total, sems):
        self.me, self.part, self.inbox, self.total, self.sems = me, part, inbox, total, sems
        return self

    def peer(self, offset):
        return lax.rem(self.me + offset, self.devices)

    def place(self, device):
        return (device // self.counts[1], lax.rem(device, self.counts[1]))

    def rows_of(self, device):
        return pl.ds(pl.multiple_of(device * self.piece, 8), self.piece)

    def is_owner(self, device, action):
        if self.owners == self.devices:
            action()
        else:
            pl.when(device < self.owners)(action)

    def greet(self):
        barrier = pltpu.get_barrier_semaphore()

        def signal(offset, carry):
            pl.semaphore_signal(
                barrier, inc=1, device_id=self.place(self.peer(offset)), device_id_type=pl.DeviceIdType.MESH
            )
            return carry

        lax.fori_loop(1, self.devices, signal, 0)

    def greeted(self):
        pl.semaphore_wait(pltpu.get_barrier_semaphore(), self.devices - 1)

    def outgoing(self, offset):
        peer = self.peer(offset)
        return pltpu.make_async_remote_copy(
            src_ref=self.part.at[self.rows_of(peer)],
            dst_ref=self.inbox.at[offset - 1],
            send_sem=self.sems.at[0],
            recv_sem=self.sems.at[1],
            device_id=self.place(peer),
            device_id_type=pl.DeviceIdType.MESH,
        )

    def spread(self, offset):
        mine = self.total.at[self.rows_of(self.me)]
        return pltpu.make_async_remote_copy(
            src_ref=mine,
            dst_ref=mine,
            send_sem=self.sems.at[2],
            recv_sem=self.sems.at[3],
            device_id=self.place(self.peer(offset)),
            device_id_type=pl.DeviceIdType.MESH,
        )

    def each_peer(self, action):
        def step(offset, carry):
            action(offset)
            return carry

        lax.fori_loop(1, self.devices, step, 0)

    def start(self):
        if self.rows > self.used:
            spare = self.rows - self.used
            self.part[pl.ds(self.used, spare), :] = jnp.zeros((spare, LANES), jnp.float32)
        self.each_peer(lambda offset: self.is_owner(self.peer(offset), lambda: self.outgoing(offset).start()))

    def reduce(self):
        def owned():
            pltpu.make_async_copy(self.inbox, self.inbox, self.sems.at[1]).wait()
            mine = self.rows_of(self.me)
            summed = self.part[mine, :]
            for slot in range(self.devices - 1):
                summed = summed + self.inbox[slot]
            self.total[mine, :] = summed
            self.each_peer(lambda offset: self.spread(offset).start())

        self.is_owner(self.me, owned)

    def wait_rows(self, rows):
        view = self.total.at[pl.ds(0, rows)]
        pltpu.make_async_copy(view, view, self.sems.at[3]).wait()

    def finish(self):
        if self.owners == self.devices:
            self.wait_rows(self.rows - self.piece)
        else:
            pl.when(self.me < self.owners)(lambda: self.wait_rows(self.rows - self.piece))
            pl.when(self.me >= self.owners)(lambda: self.wait_rows(self.rows))
        self.each_peer(lambda offset: self.is_owner(self.peer(offset), lambda: self.outgoing(offset).wait_send()))
        self.is_owner(self.me, lambda: self.each_peer(lambda offset: self.spread(offset).wait_send()))


def store_gram(part, source, pairs):
    for index, (i, j) in enumerate(pairs):
        part[block(index), :] = dot_tn(source[:, block(i)], source[:, block(j)])


def factor_block(work):
    sub, lane = iotas((PANEL, LANES))

    def step(group, carry):
        top = group * PANEL
        rows = pl.ds(pl.multiple_of(top, PANEL), PANEL)
        left = work[rows, pl.ds(0, LANES)]
        right = work[rows, pl.ds(LANES, LANES)]
        rolled = pltpu.roll(left, lax.rem(LANES - top, LANES), 1)
        cols = [jnp.broadcast_to(rolled[:, k : k + 1], (PANEL, LANES)) for k in range(PANEL)]
        scale = jnp.zeros((PANEL, LANES), jnp.float32)
        for k in range(PANEL):
            root = lax.rsqrt(cols[k][k : k + 1, :])
            scale = jnp.where(sub == k, root, scale)
            factor = jnp.where(sub > k, cols[k] * root, 0.0)
            for later in range(k + 1, PANEL):
                cols[later] = cols[later] - factor * (cols[later][k : k + 1, :] * root)
            left = left - factor * (left[k : k + 1, :] * root)
            right = right - factor * (right[k : k + 1, :] * root)
        left = jnp.where(lane >= top + sub, left * scale, 0.0)
        right = right * scale
        both = jnp.concatenate([left, right], axis=1)
        below = jnp.where(lane >= top + PANEL, left, 0.0)
        work[...] = work[...] - dot_tn(below, both)
        work[rows, :] = both
        return carry

    lax.fori_loop(0, LANES // PANEL, step, 0)


def factor_all(width, gram, work, upper, inverse, after_block=lambda b: None):
    pairs = upper_pairs(width)
    size = width * LANES
    rate = shift_frac / size
    row, lane = iotas((LANES, LANES))
    same = row == lane
    trace = jnp.float32(0.0)
    for index, (i, j) in enumerate(pairs):
        if i == j:
            trace = trace + jnp.sum(jnp.where(same, gram[block(index), :], 0.0))
    shift = rate * trace
    eye = jnp.where(same, 1.0, 0.0).astype(jnp.float32)
    zero = jnp.zeros((LANES, LANES), jnp.float32)
    for index, (i, j) in enumerate(pairs):
        piece = gram[block(index), :]
        upper[block(i), block(j)] = piece + shift * eye if i == j else piece
        if i != j:
            upper[block(j), block(i)] = zero
            inverse[block(i), block(j)] = zero
    for b in range(width):
        work[:, pl.ds(0, LANES)] = upper[block(b), block(b)]
        work[:, pl.ds(LANES, LANES)] = eye
        factor_block(work)
        upper[block(b), block(b)] = work[:, pl.ds(0, LANES)]
        inv = work[:, pl.ds(LANES, LANES)]
        inverse[block(b), block(b)] = inv
        for j in range(b + 1, width):
            upper[block(b), block(j)] = dot(inv, upper[block(b), block(j)])
        for i in range(b + 1, width):
            for j in range(i, width):
                upper[block(i), block(j)] = upper[block(i), block(j)] - dot_tn(
                    upper[block(b), block(i)], upper[block(b), block(j)]
                )
        for j in range(b):
            acc = zero
            for k in range(j, b):
                acc = acc + dot_tn(upper[block(k), block(b)], inverse[block(k), block(j)])
            inverse[block(b), block(j)] = -dot(inv, acc)
        after_block(b)


def gram_grad(upper, inverse, total_grad, rate):
    row, lane = iotas(total_grad.shape)
    lower_grad = jnp.where(row >= lane, total_grad.T, 0.0)
    product = dot(upper, lower_grad)
    phi = jnp.where(row > lane, product, jnp.where(row == lane, 0.5 * product, 0.0))
    sandwich = dot(dot_tn(inverse, phi), inverse)
    result = 0.5 * (sandwich + sandwich.T)
    trace = jnp.sum(jnp.where(row == lane, result, 0.0))
    return result + jnp.where(row == lane, rate * trace, 0.0)


def whole_kernel(counts, width, matrix, q_grad, grad_factor, out, *scratch):
    gram_sum, later_sum, cross_sum = scratch[0:4], scratch[4:8], scratch[8:12]
    work, upper1, inverse1, upper2, inverse2, current, square = scratch[12:]
    me = lax.axis_index("rows") * counts[1] + lax.axis_index("sub")
    pairs = upper_pairs(width)
    used = len(pairs) * LANES
    rate = shift_frac / (width * LANES)
    first = Summer(counts, used).bind(me, *gram_sum)
    second = Summer(counts, used).bind(me, *later_sum)
    cross = Summer(counts, width * width * LANES).bind(me, *cross_sum)

    first.greet()
    store_gram(first.part, matrix, pairs)
    first.greeted()
    first.start()
    first.reduce()
    first.finish()
    factor_all(width, first.total, work, upper1, inverse1)
    current[...] = dot_nt(matrix[...], inverse1[...])

    store_gram(second.part, current, pairs)
    second.start()
    for i in range(width):
        for j in range(width):
            cross.part[block(i * width + j), :] = dot_tn(current[:, block(i)], q_grad[:, block(j)])
    second.reduce()
    second.finish()
    cross.start()

    def after_block(b):
        if b == width - 2:
            cross.reduce()

    factor_all(width, second.total, work, upper2, inverse2, after_block)
    factor2 = dot_nt(grad_factor[...], upper1[...])
    factor1 = dot_tn(upper2[...], grad_factor[...])
    moved = dot(q_grad[...], inverse2[...])
    cross.finish()
    for i in range(width):
        for j in range(width):
            square[block(i), block(j)] = cross.total[block(i * width + j), :]
    turned = dot(square[...], inverse2[...])
    total2 = factor2 - dot(inverse2[...], turned)
    grad2 = gram_grad(upper2[...], inverse2[...], total2, rate)
    for index, (i, j) in enumerate(pairs):
        piece = second.total[block(index), :]
        square[block(i), block(j)] = piece
        if i != j:
            square[block(j), block(i)] = piece.T
    crossed1 = turned + 2.0 * dot(square[...], grad2)
    total1 = factor1 - dot(crossed1, inverse1[...])
    grad1 = gram_grad(upper1[...], inverse1[...], total1, rate)
    middle = moved + 2.0 * dot(current[...], grad2)
    out[...] = dot(middle, inverse1[...]) + 2.0 * dot(matrix[...], grad1)


def per_device(counts, matrix, grad_out, grad_factor):
    rows, size = matrix.shape
    width = size // LANES
    used = len(upper_pairs(width)) * LANES
    vmem = pl.BlockSpec(memory_space=pltpu.VMEM)
    square = pltpu.VMEM((size, size), jnp.float32)
    tall = pltpu.VMEM((rows, size), jnp.float32)
    work = pltpu.VMEM((LANES, 2 * LANES), jnp.float32)
    sums = (
        Summer(counts, used).scratch() + Summer(counts, used).scratch() + Summer(counts, width * size).scratch()
    )
    return pl.pallas_call(
        functools.partial(whole_kernel, counts, width),
        out_shape=jax.ShapeDtypeStruct((rows, size), jnp.float32),
        in_specs=[vmem] * 3,
        out_specs=vmem,
        scratch_shapes=sums + [work] + [square] * 4 + [tall, square],
        compiler_params=pltpu.CompilerParams(
            vmem_limit_bytes=VMEM_LIMIT, collective_id=0, has_side_effects=True
        ),
    )(matrix, grad_out, grad_factor)


def solution(mesh):
    counts = (mesh.shape["rows"], mesh.shape["sub"])
    placed = (P(("rows", "sub"), None), P(("rows", "sub"), None), P())
    return jax.shard_map(
        functools.partial(per_device, counts),
        mesh=mesh,
        in_specs=placed,
        out_specs=P(("rows", "sub"), None),
        check_vma=False,
    )
```

```python
import functools

import jax
import jax.numpy as jnp
from jax import lax
from jax.experimental import pallas as pl
from jax.experimental.pallas import tpu as pltpu
from jax.sharding import PartitionSpec as P

LANES = 128
PANEL = 16
shift_frac = 0.02
VMEM_LIMIT = 56 * 1024 * 1024


def dot(left, right, dims=((1,), (0,))):
    return lax.dot_general(
        left, right, (dims, ((), ())), precision=lax.Precision.HIGHEST, preferred_element_type=jnp.float32
    )


def halves(value):
    high = value.astype(jnp.bfloat16)
    return high, (value - high.astype(jnp.float32)).astype(jnp.bfloat16)


def dot3(left, right, dims=((1,), (0,))):
    (left_high, left_low), (right_high, right_low) = halves(left), halves(right)

    def product(a, b):
        return lax.dot_general(a, b, (dims, ((), ())), preferred_element_type=jnp.float32)

    return product(left_high, right_high) + (product(left_high, right_low) + product(left_low, right_high))


def dot3_tn(left, right):
    return dot3(left, right, ((0,), (0,)))


def dot3_nt(left, right):
    return dot3(left, right, ((1,), (1,)))


def dot_tn(left, right):
    return dot(left, right, ((0,), (0,)))


def dot_nt(left, right):
    return dot(left, right, ((1,), (1,)))


def upper_pairs(count):
    return [(i, j) for i in range(count) for j in range(i, count)]


def block(index):
    return pl.ds(index * LANES, LANES)


def iotas(shape):
    return lax.broadcasted_iota(jnp.int32, shape, 0), lax.broadcasted_iota(jnp.int32, shape, 1)


def piece_rows(rows, devices):
    share = -(-rows // devices)
    return -(-share // 8) * 8


class Summer:
    def __init__(self, counts, rows):
        self.counts, self.used = counts, rows
        self.devices = counts[0] * counts[1]
        self.piece = piece_rows(rows, self.devices)
        self.owners = -(-rows // self.piece)
        self.rows = self.owners * self.piece

    def scratch(self):
        return [
            pltpu.VMEM((self.rows, LANES), jnp.float32),
            pltpu.VMEM((self.devices - 1, self.piece, LANES), jnp.float32),
            pltpu.VMEM((self.rows, LANES), jnp.float32),
            pltpu.SemaphoreType.DMA((4,)),
        ]

    def bind(self, me, part, inbox, total, sems):
        self.me, self.part, self.inbox, self.total, self.sems = me, part, inbox, total, sems
        return self

    def peer(self, offset):
        return lax.rem(self.me + offset, self.devices)

    def place(self, device):
        return (device // self.counts[1], lax.rem(device, self.counts[1]))

    def rows_of(self, device):
        return pl.ds(pl.multiple_of(device * self.piece, 8), self.piece)

    def is_owner(self, device, action):
        if self.owners == self.devices:
            action()
        else:
            pl.when(device < self.owners)(action)

    def greet(self):
        barrier = pltpu.get_barrier_semaphore()

        def signal(offset, carry):
            pl.semaphore_signal(
                barrier, inc=1, device_id=self.place(self.peer(offset)), device_id_type=pl.DeviceIdType.MESH
            )
            return carry

        lax.fori_loop(1, self.devices, signal, 0)

    def greeted(self):
        pl.semaphore_wait(pltpu.get_barrier_semaphore(), self.devices - 1)

    def outgoing(self, offset):
        peer = self.peer(offset)
        return pltpu.make_async_remote_copy(
            src_ref=self.part.at[self.rows_of(peer)],
            dst_ref=self.inbox.at[offset - 1],
            send_sem=self.sems.at[0],
            recv_sem=self.sems.at[1],
            device_id=self.place(peer),
            device_id_type=pl.DeviceIdType.MESH,
        )

    def spread(self, offset):
        mine = self.total.at[self.rows_of(self.me)]
        return pltpu.make_async_remote_copy(
            src_ref=mine,
            dst_ref=mine,
            send_sem=self.sems.at[2],
            recv_sem=self.sems.at[3],
            device_id=self.place(self.peer(offset)),
            device_id_type=pl.DeviceIdType.MESH,
        )

    def each_peer(self, action):
        def step(offset, carry):
            action(offset)
            return carry

        lax.fori_loop(1, self.devices, step, 0)

    def start(self):
        if self.rows > self.used:
            spare = self.rows - self.used
            self.part[pl.ds(self.used, spare), :] = jnp.zeros((spare, LANES), jnp.float32)
        self.each_peer(lambda offset: self.is_owner(self.peer(offset), lambda: self.outgoing(offset).start()))

    def reduce(self):
        def owned():
            pltpu.make_async_copy(self.inbox, self.inbox, self.sems.at[1]).wait()
            mine = self.rows_of(self.me)
            summed = self.part[mine, :]
            for slot in range(self.devices - 1):
                summed = summed + self.inbox[slot]
            self.total[mine, :] = summed
            self.each_peer(lambda offset: self.spread(offset).start())

        self.is_owner(self.me, owned)

    def wait_rows(self, rows):
        view = self.total.at[pl.ds(0, rows)]
        pltpu.make_async_copy(view, view, self.sems.at[3]).wait()

    def finish(self):
        if self.owners == self.devices:
            self.wait_rows(self.rows - self.piece)
        else:
            pl.when(self.me < self.owners)(lambda: self.wait_rows(self.rows - self.piece))
            pl.when(self.me >= self.owners)(lambda: self.wait_rows(self.rows))
        self.each_peer(lambda offset: self.is_owner(self.peer(offset), lambda: self.outgoing(offset).wait_send()))
        self.is_owner(self.me, lambda: self.each_peer(lambda offset: self.spread(offset).wait_send()))


def store_gram(part, source, pairs):
    for index, (i, j) in enumerate(pairs):
        part[block(index), :] = dot_tn(source[:, block(i)], source[:, block(j)])


def factor_block(work):
    sub, lane = iotas((PANEL, LANES))

    def step(group, carry):
        top = group * PANEL
        rows = pl.ds(pl.multiple_of(top, PANEL), PANEL)
        waiting, source = carry
        turn = lax.rem(LANES - top, LANES)
        others = work[...] - dot_tn(waiting, source)
        ahead = pltpu.roll(waiting, turn, 1)[:, 0:PANEL]
        panel = work[rows, :] - dot_tn(ahead, source)
        left, right = panel[:, 0:LANES], panel[:, LANES:]
        rolled = pltpu.roll(left, turn, 1)
        cols = [jnp.broadcast_to(rolled[:, k : k + 1], (PANEL, LANES)) for k in range(PANEL)]
        scale = jnp.zeros((PANEL, LANES), jnp.float32)
        for k in range(PANEL):
            root = lax.rsqrt(cols[k][k : k + 1, :])
            scale = jnp.where(sub == k, root, scale)
            factor = jnp.where(sub > k, cols[k] * root, 0.0)
            for later in range(k + 1, PANEL):
                cols[later] = cols[later] - factor * (cols[later][k : k + 1, :] * root)
            left = left - factor * (left[k : k + 1, :] * root)
            right = right - factor * (right[k : k + 1, :] * root)
        left = jnp.where(lane >= top + sub, left * scale, 0.0)
        right = right * scale
        both = jnp.concatenate([left, right], axis=1)
        below = jnp.where(lane >= top + PANEL, left, 0.0)
        work[...] = others
        work[rows, :] = both
        return below, both

    none = jnp.zeros((PANEL, LANES), jnp.float32), jnp.zeros((PANEL, 2 * LANES), jnp.float32)
    lax.fori_loop(0, LANES // PANEL, step, none)


def factor_all(width, gram, work, upper, inverse, after_block=lambda b: None):
    pairs = upper_pairs(width)
    size = width * LANES
    rate = shift_frac / size
    row, lane = iotas((LANES, LANES))
    same = row == lane
    trace = jnp.float32(0.0)
    for index, (i, j) in enumerate(pairs):
        if i == j:
            trace = trace + jnp.sum(jnp.where(same, gram[block(index), :], 0.0))
    shift = rate * trace
    eye = jnp.where(same, 1.0, 0.0).astype(jnp.float32)
    zero = jnp.zeros((LANES, LANES), jnp.float32)
    for index, (i, j) in enumerate(pairs):
        piece = gram[block(index), :]
        upper[block(i), block(j)] = piece + shift * eye if i == j else piece
        if i != j:
            upper[block(j), block(i)] = zero
            inverse[block(i), block(j)] = zero
    for b in range(width):
        work[:, pl.ds(0, LANES)] = upper[block(b), block(b)]
        work[:, pl.ds(LANES, LANES)] = eye
        factor_block(work)
        upper[block(b), block(b)] = work[:, pl.ds(0, LANES)]
        inv = work[:, pl.ds(LANES, LANES)]
        inverse[block(b), block(b)] = inv
        for j in range(b + 1, width):
            upper[block(b), block(j)] = dot(inv, upper[block(b), block(j)])
        for i in range(b + 1, width):
            for j in range(i, width):
                upper[block(i), block(j)] = upper[block(i), block(j)] - dot_tn(
                    upper[block(b), block(i)], upper[block(b), block(j)]
                )
        for j in range(b):
            acc = zero
            for k in range(j, b):
                acc = acc + dot_tn(upper[block(k), block(b)], inverse[block(k), block(j)])
            inverse[block(b), block(j)] = -dot(inv, acc)
        after_block(b)


def gram_grad(upper, inverse, total_grad, rate):
    row, lane = iotas(total_grad.shape)
    lower_grad = jnp.where(row >= lane, total_grad.T, 0.0)
    product = dot3(upper, lower_grad)
    phi = jnp.where(row > lane, product, jnp.where(row == lane, 0.5 * product, 0.0))
    sandwich = dot3(dot3_tn(inverse, phi), inverse)
    result = 0.5 * (sandwich + sandwich.T)
    trace = jnp.sum(jnp.where(row == lane, result, 0.0))
    return result + jnp.where(row == lane, rate * trace, 0.0)


def whole_kernel(counts, width, matrix, q_grad, grad_factor, out, *scratch):
    gram_sum, later_sum, cross_sum = scratch[0:4], scratch[4:8], scratch[8:12]
    work, upper1, inverse1, upper2, inverse2, current, square, held = scratch[12:]
    me = lax.axis_index("rows") * counts[1] + lax.axis_index("sub")
    pairs = upper_pairs(width)
    used = len(pairs) * LANES
    rate = shift_frac / (width * LANES)
    first = Summer(counts, used).bind(me, *gram_sum)
    second = Summer(counts, used).bind(me, *later_sum)
    cross = Summer(counts, width * width * LANES).bind(me, *cross_sum)

    first.greet()
    store_gram(first.part, matrix, pairs)
    first.greeted()
    first.start()
    first.reduce()
    first.finish()
    factor_all(width, first.total, work, upper1, inverse1)
    current[...] = dot_nt(matrix[...], inverse1[...])

    store_gram(second.part, current, pairs)
    second.start()
    for i in range(width):
        for j in range(width):
            cross.part[block(i * width + j), :] = dot_tn(current[:, block(i)], q_grad[:, block(j)])
    held[...] = dot3_nt(grad_factor[...], upper1[...])
    second.reduce()
    second.finish()
    cross.start()

    def after_block(b):
        if b == width - 2:
            cross.reduce()

    factor_all(width, second.total, work, upper2, inverse2, after_block)
    factor1 = dot3_tn(upper2[...], grad_factor[...])
    moved = dot3(q_grad[...], inverse2[...])
    cross.finish()
    for i in range(width):
        for j in range(width):
            square[block(i), block(j)] = cross.total[block(i * width + j), :]
    turned = dot3(square[...], inverse2[...])
    total2 = held[...] - dot3(inverse2[...], turned)
    grad2 = gram_grad(upper2[...], inverse2[...], total2, rate)
    for index, (i, j) in enumerate(pairs):
        piece = second.total[block(index), :]
        square[block(i), block(j)] = piece
        if i != j:
            square[block(j), block(i)] = piece.T
    crossed1 = turned + 2.0 * dot3(square[...], grad2)
    total1 = factor1 - dot3(crossed1, inverse1[...])
    grad1 = gram_grad(upper1[...], inverse1[...], total1, rate)
    middle = moved + 2.0 * dot3(current[...], grad2)
    out[...] = dot3(middle, inverse1[...]) + 2.0 * dot3(matrix[...], grad1)


def per_device(counts, matrix, grad_out, grad_factor):
    rows, size = matrix.shape
    width = size // LANES
    used = len(upper_pairs(width)) * LANES
    vmem = pl.BlockSpec(memory_space=pltpu.VMEM)
    square = pltpu.VMEM((size, size), jnp.float32)
    tall = pltpu.VMEM((rows, size), jnp.float32)
    work = pltpu.VMEM((LANES, 2 * LANES), jnp.float32)
    sums = (
        Summer(counts, used).scratch() + Summer(counts, used).scratch() + Summer(counts, width * size).scratch()
    )
    return pl.pallas_call(
        functools.partial(whole_kernel, counts, width),
        out_shape=jax.ShapeDtypeStruct((rows, size), jnp.float32),
        in_specs=[vmem] * 3,
        out_specs=vmem,
        scratch_shapes=sums + [work] + [square] * 4 + [tall, square, square],
        compiler_params=pltpu.CompilerParams(
            vmem_limit_bytes=VMEM_LIMIT, collective_id=0, has_side_effects=True
        ),
    )(matrix, grad_out, grad_factor)


def solution(mesh):
    counts = (mesh.shape["rows"], mesh.shape["sub"])
    placed = (P(("rows", "sub"), None), P(("rows", "sub"), None), P())
    return jax.shard_map(
        functools.partial(per_device, counts),
        mesh=mesh,
        in_specs=placed,
        out_specs=P(("rows", "sub"), None),
        check_vma=False,
    )
```
